32 devices in a mesh: tp: 4 (over x, core), fsdp: 8 (over z, y).
Axes of the slice: x: 2, y: 2, z: 4, core: 2. Of those that a mesh axis runs over, the one named last changes fastest.
Arguments:
- sectioned: bfloat16 [64, 256, 26624], P('fsdp', None, 'tp'), as said below
- loader_owner: int32 [64], replicated, may hold values from 0 to 7, as said below
- slab_order: int32 [64], replicated, may hold values from 0 to 7, as said below
Outputs:
- dequant: bfloat16 [16384, 26624], P(('tp', 'fsdp'))
- scale_codes: float32 [26624, 256], P(('tp', 'fsdp'))
- group_max: float32 [26624], P(('tp', 'fsdp'))
The draws below stay inside these ranges and needn't reach their ends.
Inputs may be any that keep to these rules, and one draw needn't show every extreme that they name: `loader_owner`: slab s holds rows s * 256 to (s + 1) * 256 - 1; for each f, the 8 slabs s with (s // 2) % 8 == f have 8 distinct owners. `slab_order`: the slabs of one owner have distinct orders. `sectioned`: entries are finite.
All inputs are finite; a program needn't handle non-finite values. Where the reference program divides by a largest or mean magnitude, that divisor is 1e-20 or more.
Results may differ from the reference program's by a relative error of at most 0.0015.
Values may be sent and summed in bfloat16 or wider, within the bound.
A program may use at most 256 MiB of HBM per device.

```python
import jax
import jax.numpy as jnp
from jax import lax

D = 16384
FFW = 26624
OWNERS = 8
SLABS = 64
SR = 256
SPB = 2
N_TP = 4
N_FSDP = 8


def loader_layout(key):
    first = jax.random.fold_in(key, 11)
    second = jax.random.fold_in(key, 12)
    rng = jnp.arange(N_FSDP)
    owners = jax.vmap(lambda f: jax.random.permutation(jax.random.fold_in(first, f), N_FSDP))(rng)
    slots = jax.vmap(lambda o: jax.random.permutation(jax.random.fold_in(second, o), N_FSDP))(rng)
    slab = jnp.arange(SLABS)
    block = slab // SPB
    target = block % N_FSDP
    place = block // N_FSDP * SPB + slab % SPB
    owner = owners[target, place]
    order = slots[owner, target]
    return (owner.astype(jnp.int32), order.astype(jnp.int32))


def draw_loader_owner(key, part):
    return loader_layout(key)[0]


def draw_slab_order(key, part):
    return loader_layout(key)[1]


def draw_sectioned(key, part):
    owner, order = loader_layout(key)
    slot = owner * N_FSDP + order
    slab_at = jnp.zeros((SLABS,), jnp.int32).at[slot].set(jnp.arange(SLABS, dtype=jnp.int32))
    owner_of_slot = (jnp.arange(SLABS) // N_FSDP).astype(jnp.float32)
    block_pos = (slab_at // SPB).astype(jnp.float32)
    level = jnp.exp(jnp.log(3.0) * (owner_of_slot / max(N_FSDP - 1, 1) + block_pos / max(N_TP * N_FSDP - 1, 1)))
    noise_key = jax.random.fold_in(key, 13)
    values = jax.random.normal(noise_key, (SLABS, SR, FFW), jnp.float32) * 0.5
    return (values * level[:, None, None]).astype(jnp.bfloat16)


def setup_inputs(seed: int = 0) -> dict:
    seeds = jax.random.split(jax.random.key(seed), 4)
    sectioned = draw_sectioned(jax.random.fold_in(seeds[3], 71), 0)
    loader_owner = draw_loader_owner(jax.random.fold_in(seeds[3], 71), 0)
    slab_order = draw_slab_order(jax.random.fold_in(seeds[3], 71), 0)
    return {"sectioned": sectioned, "loader_owner": loader_owner, "slab_order": slab_order}


LEVELS = [-1.0, -0.6961928009986877, -0.5250730514526367, -0.39491748809814453,
          -0.28444138169288635, -0.18477343022823334, -0.09105003625154495, 0.0,
          0.07958029955625534, 0.16093020141124725, 0.24611230194568634, 0.33791524171829224,
          0.44070982933044434, 0.5626170039176941, 0.7229568362236023, 1.0]
MIDPOINTS = [(LEVELS[k] + LEVELS[k + 1]) / 2.0 for k in range(15)]
STEPSIZES = [LEVELS[k + 1] - LEVELS[k] for k in range(15)]
EPS = 1e-6


def hard_code(block):
    values = block.astype(jnp.float32)
    shape = values.shape
    grouped = values.reshape(shape[:-1] + (shape[-1] // 64, 64))
    absmax = jnp.max(jnp.abs(grouped), axis=-1)
    spread = jnp.repeat(absmax, 64, axis=-1)
    ratio = values / (spread + EPS)
    level = jnp.full(shape, LEVELS[0], jnp.float32)
    for middle, stepsize in zip(MIDPOINTS, STEPSIZES):
        level = level + jnp.where(ratio > middle, stepsize, 0.0).astype(jnp.float32)
    coded = (spread * level).astype(jnp.bfloat16)
    return coded, absmax


def reference(sectioned, loader_owner, slab_order):
    slot = (loader_owner * OWNERS + slab_order).astype(jnp.int32)
    weight = jnp.take(sectioned, slot, axis=0).reshape(64, D // 64, FFW)
    coded, absmax = lax.map(hard_code, weight)
    dequant = coded.reshape(D, FFW)
    absmax = absmax.reshape(D, FFW // 64)
    offset = jnp.sum(absmax) / float(D * FFW // 64)
    centred = absmax.reshape(-1, 256) - offset
    group_max = jnp.max(jnp.abs(centred), axis=1)
    scale_codes = centred / (group_max[:, None] + EPS)
    return dequant, scale_codes, group_max
```

```python
import functools

import jax
import jax.numpy as jnp
import numpy as np
from jax import lax
from jax.experimental import pallas as pl
from jax.experimental.pallas import tpu as pltpu
from jax.sharding import PartitionSpec as P

LEVELS = [
    -1.0,
    -0.6961928009986877,
    -0.5250730514526367,
    -0.39491748809814453,
    -0.28444138169288635,
    -0.18477343022823334,
    -0.09105003625154495,
    0.0,
    0.07958029955625534,
    0.16093020141124725,
    0.24611230194568634,
    0.33791524171829224,
    0.44070982933044434,
    0.5626170039176941,
    0.7229568362236023,
    1.0,
]
MIDPOINTS = [(LEVELS[k] + LEVELS[k + 1]) / 2.0 for k in range(15)]
STEPSIZES = [LEVELS[k + 1] - LEVELS[k] for k in range(15)]
EPS = 1e-06
LANES = 128
BLOCK = 64
MESH = pl.DeviceIdType.MESH


def reached_levels():
    total = np.float32(LEVELS[0])
    reached = [float(total)]
    for step in STEPSIZES:
        total = np.float32(total + np.float32(step))
        reached.append(float(total))
    return reached


REACHED = reached_levels()


def code_tile(w):
    lane = lax.broadcasted_iota(jnp.int32, w.shape, 1)
    top = jnp.abs(w)
    low = lane < BLOCK
    first = jnp.broadcast_to(jnp.max(jnp.where(low, top, 0.0), axis=1, keepdims=True), w.shape)
    second = jnp.broadcast_to(jnp.max(jnp.where(low, 0.0, top), axis=1, keepdims=True), w.shape)
    spread = jnp.where(lane < BLOCK, first, second)
    ratio = w / (spread + EPS)
    level = jnp.full(w.shape, REACHED[0], jnp.float32)
    for middle, value in zip(MIDPOINTS, REACHED[1:]):
        level = jnp.where(ratio > middle, value, level)
    return spread * level, first, second


def exchange(
    sizes, from_owner, outgoing, out, scales, sums, arrive, coded, tops, s1, r1, l1, s2, r2, l2, sa, ra, la,
    mine, ours, got, met, sm, rm, so, ro, stage,
):
    owners, tp, chunks, rows, per_block, columns, depth = sizes
    t = lax.axis_index("tp")
    f = lax.axis_index("fsdp")
    groups = columns // LANES
    width = next(u for u in range(13, 0, -1) if groups % u == 0)

    barrier = pltpu.get_barrier_semaphore()
    for d in range(1, owners):
        pl.semaphore_signal(barrier, inc=1, device_id={"fsdp": lax.rem(f + d, owners)}, device_id_type=MESH)
    for e in range(1, tp):
        pl.semaphore_signal(barrier, inc=1, device_id={"tp": lax.rem(t + e, tp)}, device_id_type=MESH)
    pl.semaphore_wait(barrier, owners - 1 + tp - 1)

    def span(c):
        return pl.ds(pl.multiple_of(c * rows, rows), rows)

    def first_hop(c, d):
        to = lax.rem(f + d, owners)
        return pltpu.make_async_remote_copy(
            src_ref=outgoing.at[to, span(c)],
            dst_ref=arrive.at[c, f],
            send_sem=s1.at[c, d],
            recv_sem=r1.at[c, d],
            device_id={"fsdp": to},
            device_id_type=MESH,
        )

    def first_stay(c):
        return pltpu.make_async_copy(outgoing.at[f, span(c)], arrive.at[c, f], l1.at[c])

    def start_chunk(c):
        for d in range(1, owners):
            first_hop(c, d).start()
        first_stay(c).start()

    def second_hop(c, slot, e):
        to = lax.rem(t + e, tp)
        band = pl.ds(pl.multiple_of(t * columns, LANES), columns)
        data = pltpu.make_async_remote_copy(
            src_ref=coded.at[slot, to],
            dst_ref=out.at[:, span(c), band],
            send_sem=s2.at[slot, e],
            recv_sem=r2.at[c, e],
            device_id={"tp": to},
            device_id_type=MESH,
        )
        top = pltpu.make_async_remote_copy(
            src_ref=tops.at[to, :, span(c)],
            dst_ref=scales.at[t, :, span(c)],
            send_sem=sa.at[slot, e],
            recv_sem=ra.at[c, e],
            device_id={"tp": to},
            device_id_type=MESH,
        )
        return data, top

    def second_stay(c, slot):
        band = pl.ds(pl.multiple_of(t * columns, LANES), columns)
        data = pltpu.make_async_copy(coded.at[slot, t], out.at[:, span(c), band], l2.at[slot])
        top = pltpu.make_async_copy(tops.at[t, :, span(c)], scales.at[t, :, span(c)], la.at[slot])
        return data, top

    def drain(c, slot):
        for e in range(1, tp):
            for copy in second_hop(c, slot, e):
                copy.wait_send()
        for copy in second_stay(c, slot):
            copy.wait()

    def code(c, slot, to):
        lane = lax.broadcasted_iota(jnp.int32, (rows, LANES), 1)

        def place(k, _):
            owner = from_owner[to * per_block + k]

            def step(g, held):
                at = pl.multiple_of(g * (width * LANES), width * LANES)
                w = stage[owner, :, pl.ds(at, width * LANES)].astype(jnp.float32)
                made = []
                for j in range(width):
                    value, first, second = code_tile(w[:, j * LANES : (j + 1) * LANES])
                    made.append(value.astype(jnp.bfloat16))
                    index = 2 * (g * width + j)
                    held = jnp.where(lane == index, first, jnp.where(lane == index + 1, second, held))
                coded[slot, to, k, :, pl.ds(at, width * LANES)] = jnp.concatenate(made, axis=1)
                return held

            held = lax.fori_loop(0, groups // width, step, jnp.zeros((rows, LANES), jnp.float32))
            tops[to, k, span(c), :] = held
            mine[...] += held
            return 0

        lax.fori_loop(0, per_block, place, 0)

    def sum_hop(d):
        return pltpu.make_async_remote_copy(
            src_ref=mine,
            dst_ref=got.at[d],
            send_sem=sm.at[d],
            recv_sem=rm.at[d],
            device_id={"fsdp": lax.rem(f + d, owners)},
            device_id_type=MESH,
        )

    def sum_turn(e):
        return pltpu.make_async_remote_copy(
            src_ref=ours,
            dst_ref=met.at[e],
            send_sem=so.at[e],
            recv_sem=ro.at[e],
            device_id={"tp": lax.rem(t + e, tp)},
            device_id_type=MESH,
        )

    for c in range(min(depth, chunks)):
        start_chunk(c)
    mine[...] = jnp.zeros_like(mine)

    def chunk(c, _):
        slot = lax.rem(c, 2)
        for d in range(1, owners):
            first_hop(c, d).wait_recv()
        first_stay(c).wait()

        @pl.when(c + depth < chunks)
        def _():
            start_chunk(c + depth)

        @pl.when(c >= 2)
        def _():
            drain(c - 2, slot)

        def take(o, _):
            stage[o] = arrive[c, o]
            return 0

        lax.fori_loop(0, owners, take, 0)
        for e in range(1, tp + 1):
            code(c, slot, lax.rem(t + e, tp))
            if e > 1:
                for copy in second_hop(c, slot, e - 1):
                    copy.start()
        for copy in second_stay(c, slot):
            copy.start()
        return 0

    lax.fori_loop(0, chunks, chunk, 0)

    if chunks > 1:
        drain(chunks - 2, chunks % 2)
    for d in range(1, owners):
        sum_hop(d).start()
    drain(chunks - 1, (chunks - 1) % 2)
    for d in range(1, owners):
        sum_hop(d).wait()
    total = mine[...]
    for d in range(1, owners):
        total = total + got[d]
    ours[...] = total

    def finish(c, _):
        for d in range(1, owners):
            first_hop(c, d).wait_send()
        for e in range(1, tp):
            for copy in second_hop(c, 0, e):
                copy.wait_recv()
        return 0

    lax.fori_loop(0, chunks, finish, 0)
    for e in range(1, tp):
        sum_turn(e).start()
    for e in range(1, tp):
        sum_turn(e).wait()
    total = ours[...]
    for e in range(1, tp):
        total = total + met[e]
    sums[...] = total


def copy_block(*refs):
    refs[-1][...] = refs[-2][...]


def pick_slots(sectioned, send_slot):
    slots, slab_rows, columns = sectioned.shape
    rows = min(128, slab_rows)
    return pl.pallas_call(
        copy_block,
        grid_spec=pltpu.PrefetchScalarGridSpec(
            num_scalar_prefetch=1,
            grid=(slots, slab_rows // rows),
            in_specs=[pl.BlockSpec((1, rows, columns), lambda i, r, slot: (slot[i], r, 0))],
            out_specs=pl.BlockSpec((1, rows, columns), lambda i, r, slot: (i, r, 0)),
        ),
        out_shape=jax.ShapeDtypeStruct(sectioned.shape, sectioned.dtype),
        name="pick_slots",
    )(send_slot, sectioned)


def settle(values):
    total, columns = values.shape
    rows = next(r for r in (32, 16, 8) if total % r == 0)
    return pl.pallas_call(
        copy_block,
        grid=(total // rows,),
        in_specs=[pl.BlockSpec((rows, columns), lambda i: (i, 0))],
        out_specs=pl.BlockSpec((rows, columns), lambda i: (i, 0)),
        out_shape=jax.ShapeDtypeStruct(values.shape, values.dtype),
        name="settle",
    )(values)


def per_device(sectioned, loader_owner, slab_order):
    owners = lax.axis_size("fsdp")
    tp = lax.axis_size("tp")
    myself = lax.axis_index("fsdp")
    slots, slab_rows, columns = sectioned.shape
    slab_count = loader_owner.shape[0]
    per_block = owners // tp
    slab_ids = jnp.arange(slab_count, dtype=jnp.int32)
    target = slab_ids // per_block % owners
    held = loader_owner == myself
    place = jnp.arange(owners, dtype=jnp.int32)
    picks = (target[None, :] == place[:, None]) & held[None, :]
    send_slot = jnp.sum(jnp.where(picks, slab_order[None, :], 0), axis=1)
    wanted = (place // per_block * owners + myself) * per_block + place % per_block
    sought = wanted[:, None] == slab_ids[None, :]
    from_owner = jnp.sum(jnp.where(sought, loader_owner[None, :], 0), axis=1)

    outgoing = pick_slots(sectioned, send_slot)
    rows = min(16, slab_rows)
    chunks = slab_rows // rows
    blocks = columns // BLOCK
    sizes = (owners, tp, chunks, rows, per_block, columns, 4)
    dma = pltpu.SemaphoreType.DMA
    anywhere = pl.BlockSpec(memory_space=pl.ANY)
    coded, scales, sums = pl.pallas_call(
        functools.partial(exchange, sizes),
        out_shape=(
            jax.ShapeDtypeStruct((per_block, slab_rows, tp * columns), jnp.bfloat16),
            jax.ShapeDtypeStruct((tp, per_block, slab_rows, LANES), jnp.float32),
            jax.ShapeDtypeStruct((rows, LANES), jnp.float32),
        ),
        in_specs=[pl.BlockSpec(memory_space=pltpu.SMEM), anywhere],
        out_specs=(anywhere, anywhere, pl.BlockSpec(memory_space=pltpu.VMEM)),
        scratch_shapes=[
            pltpu.VMEM((chunks, owners, rows, columns), jnp.bfloat16),
            pltpu.VMEM((2, tp, per_block, rows, columns), jnp.bfloat16),
            pltpu.VMEM((tp, per_block, slab_rows, LANES), jnp.float32),
            dma((chunks, owners)),
            dma((chunks, owners)),
            dma((chunks,)),
            dma((2, tp)),
            dma((chunks, tp)),
            dma((2,)),
            dma((2, tp)),
            dma((chunks, tp)),
            dma((2,)),
            pltpu.VMEM((rows, LANES), jnp.float32),
            pltpu.VMEM((rows, LANES), jnp.float32),
            pltpu.VMEM((owners, rows, LANES), jnp.float32),
            pltpu.VMEM((tp, rows, LANES), jnp.float32),
            dma((owners,)),
            dma((owners,)),
            dma((tp,)),
            dma((tp,)),
            pltpu.VMEM((owners, rows, columns), jnp.bfloat16),
        ],
        compiler_params=pltpu.CompilerParams(
            collective_id=0, has_side_effects=True, vmem_limit_bytes=56 * 1024 * 1024
        ),
        name="exchange",
    )(from_owner, outgoing)
    dequant = settle(coded.reshape(per_block * slab_rows, tp * columns))
    absmax = jnp.transpose(scales[..., :blocks], (1, 2, 0, 3)).reshape(-1, 256)
    offset = jnp.sum(sums) / float(slab_count * slab_rows * tp * blocks)
    centred = absmax - offset
    group_max = jnp.max(jnp.abs(centred), axis=1)
    scale_codes = centred / (group_max[:, None] + EPS)
    return (dequant, scale_codes, group_max)


def solution(mesh):
    return jax.shard_map(
        per_device,
        mesh=mesh,
        in_specs=(P("fsdp", None, "tp"), P(), P()),
        out_specs=(P(("tp", "fsdp"), None), P(("tp", "fsdp"), None), P(("tp", "fsdp"))),
        check_vma=False,
    )
```
